32 devices in a mesh: pipe: 4 (over y, core), vocab: 2 (over x), expert: 4 (over z).
Axes of the slice: x: 2, y: 2, z: 4, core: 2. Of those that a mesh axis runs over, the one named last changes fastest.
Arguments:
- token_ids: int32 [192], replicated, may hold values from 0 to 65535
- routes: int32 [192, 2], replicated, may hold values from 0 to 3, all different within a row; in each aligned block of 192 rows (0 to 191, 192 to 383, ...) at most 144 rows name the same one
- gate_weights: float32 [192, 2], replicated, may hold values from 0.2 to 1
- embed_table: bfloat16 [65536, 7168], P(('pipe', 'vocab'), 'expert'), may hold values from -0.59765625 to 0.59765625
- w_gate: bfloat16 [4, 7168, 2048], P('expert', None, ('pipe', 'vocab')), may hold values from -0.5 to 0.5
- w_up: bfloat16 [4, 7168, 2048], P('expert', None, ('pipe', 'vocab')), may hold values from -0.5 to 0.5
- w_down: bfloat16 [4, 2048, 7168], P('expert', ('pipe', 'vocab')), may hold values from -0.125 to 0.125
Outputs:
- logits: bfloat16 [192, 65536], P('expert', ('pipe', 'vocab'))
The draws below stay inside these ranges and needn't reach their ends.
Inputs may be any that keep to these rules, and one draw needn't show every extreme that they name: `routes`: each row names 2 different experts; over all 192 rows no expert is named more than 144 times, a bound that some block reaches.
All inputs are finite; a program needn't handle non-finite values.
Results may differ from the reference program's by a relative error of at most 0.025.
Values may be sent and summed in bfloat16 or wider, within the bound.
A program may use at most 128 MiB of HBM per device.

```python
import math
import jax
import jax.numpy as jnp
import numpy as np
from jax import lax

D = 7168
FF = 2048
VOC = 65536
TOPK = 2
EXPERTS = 4
TOKENS = 192
CAP = 144
N_EXPERT = 4


def set_ends(entries, stream_key, smallest, largest):
    shape = entries.shape
    spot = [jax.random.randint(jax.random.fold_in(stream_key, axis), (), 0, shape[axis]) for axis in range(len(shape))]
    entries = entries.at[tuple(spot)].set(smallest)
    longest = shape.index(max(shape))
    spot[longest] = (spot[longest] + 1) % shape[longest]
    return entries.at[tuple(spot)].set(largest)


def shard_levels(key, shape, split, low, largest):
    gain, own = 1.0, jax.random.fold_in(key, 6)
    for axis_at, blocks in split:
        draws = jnp.exp(jax.random.uniform(jax.random.fold_in(own, axis_at), (blocks,), jnp.float32, low / len(split), largest / len(split)))
        gain = gain * jnp.repeat(draws, shape[axis_at] // blocks).reshape([-1 if axis == axis_at else 1 for axis in range(len(shape))])
    return gain


def cumulative_ranks(count, lean):
    weights = [(1 << 20) // math.isqrt(rank ** lean) + 1 for rank in range(1, count + 1)]
    width = 1 + sum(weights) // (1 << 30)
    return np.cumsum(np.array([max(1, weight // width) for weight in weights]))


def ranked(key, extent, count, slope):
    grid = cumulative_ranks(count, slope)
    pick = jax.random.randint(jax.random.fold_in(key, 1), extent, 0, int(grid[count - 1]))
    grade = jnp.searchsorted(jnp.asarray(grid, jnp.int32), pick, side="right")
    return jax.random.permutation(jax.random.fold_in(key, 2), count)[grade].astype(jnp.int32)


def shared_out(key, own, number, rows, amount, top, reach, slope):
    ranking = jax.random.permutation(key, amount)
    packed, usual = portions_of(amount, rows * top, reach, slope, True), portions_of(amount, rows * top, reach, slope, False)
    places = jnp.arange(amount)

    def named(tallies, turn):
        used = int((tallies > 0).sum())
        fixed = max(1, used // 4)
        passed = fixed + (places - fixed + turn * (used - fixed)) % max(1, amount - fixed)
        return jnp.zeros((amount,), jnp.int32).at[ranking[jnp.where(places < fixed, places, passed)]].set(jnp.asarray(tallies, jnp.int32))

    tallies = jnp.where(number % 4 == 0, named(packed, number // 4), named(usual, number - number // 4 - 1))
    mixed = jax.random.permutation(jax.random.fold_in(own, 3), amount)
    giver, sink = mixed[0:amount // 2 * 2:2], mixed[1:amount // 2 * 2:2]
    margin = jnp.minimum(tallies[giver] - 1, reach - tallies[sink]) // 2
    margin = jnp.where((giver == ranking[0]) | (sink == ranking[0]) | (tallies[sink] == 0), 0, jnp.maximum(margin, 0))
    passed = jax.random.randint(jax.random.fold_in(own, 4), (amount // 2,), 0, 1 << 20) % (margin + 1)
    tallies = tallies.at[giver].add(-passed).at[sink].add(passed)
    members = jnp.searchsorted(jnp.cumsum(tallies), jnp.arange(rows * top), side="right").astype(jnp.int32)
    listing = members.reshape(top, rows).T
    listing = listing[jax.random.permutation(jax.random.fold_in(own, 1), rows)]
    turn = jax.random.randint(jax.random.fold_in(own, 2), (rows, 1), 0, top)
    return jnp.take_along_axis(listing, (jnp.arange(top)[None, :] + turn) % top, axis=1)


def portions_of(number_of, total, most, slope, full):
    loads = [(1 << 20) // math.isqrt(rank ** slope) + 1 for rank in range(1, number_of + 1)]
    largest = most if full else min(most, max(-(-total // number_of), total * loads[0] // sum(loads)))
    least = 1 if total - largest >= number_of - 1 else 0
    given, spare = [largest] + [least] * (number_of - 1), total - largest - least * (number_of - 1)
    while spare > 0:
        candidates = [i for i in range(1, number_of) if given[i] < largest] or [i for i in range(1, number_of) if given[i] < most]
        whole, budget = sum([loads[i] for i in candidates]), spare
        for i in candidates:
            more = min(most - given[i], max(1, budget * loads[i] // whole), spare)
            given[i] = given[i] + more
            spare = spare - more
    return np.array(given)


def normal_values(key, dims, width, reach, cuts=(), held_as=jnp.bfloat16):
    result = jax.random.normal(key, dims, jnp.float32) * width
    if len(cuts) > 0:
        result = shard_levels(key, dims, cuts, -0.22, 0.18) * result
    return jnp.clip(result, min=-reach, max=reach).astype(held_as)


def setup_inputs(seed: int = 0) -> dict:
    streams_of = jax.random.split(jax.random.key(seed), 8)
    token_ids = set_ends(ranked(streams_of[0], (TOKENS,), VOC, 2), jax.random.fold_in(streams_of[0], 3), 0, VOC - 1).astype(jnp.int32)
    routes_keys = jax.random.split(jax.random.fold_in(streams_of[1], 1), TOKENS // TOKENS)
    routes_turns = jax.random.permutation(jax.random.fold_in(streams_of[1], 3), TOKENS // TOKENS)
    routes = jax.vmap(lambda own, number: shared_out(jax.random.fold_in(streams_of[1], 2), own, number, TOKENS, EXPERTS, TOPK, CAP, 1))(routes_keys, routes_turns).reshape((TOKENS, TOPK))
    gate_weights = jnp.clip(jax.random.uniform(streams_of[2], (TOKENS, TOPK), jnp.float32, 0.2, 1.0), 0.2, 1.0)
    embed_table = normal_values(streams_of[3], (VOC, D), 0.1, 0.59765625, ((0, 8), (1, 4)))
    w_gate = normal_values(streams_of[4], (EXPERTS, D, FF), (D // 64) ** -0.5, 0.5, ((0, 4), (2, 8)))
    w_up = normal_values(streams_of[5], (EXPERTS, D, FF), (D // 64) ** -0.5, 0.5, ((0, 4), (2, 8)))
    w_down = normal_values(streams_of[6], (EXPERTS, FF, D), FF ** -0.5, 0.125, ((0, 4), (1, 8)))
    return {"token_ids": token_ids, "routes": routes, "gate_weights": gate_weights, "embed_table": embed_table, "w_gate": w_gate, "w_up": w_up, "w_down": w_down}


def reference(token_ids, routes, gate_weights, embed_table, w_gate, w_up, w_down):
    embedded = embed_table[token_ids]
    flat_routes = routes.reshape(-1)
    one_hot = (flat_routes[:, None] == jnp.arange(EXPERTS, dtype=jnp.int32)[None, :]).astype(jnp.int32)
    slot_index = jnp.sum((jnp.cumsum(one_hot, axis=0) - one_hot) * one_hot, axis=1).astype(jnp.int32)
    slot_dest = (flat_routes * CAP + slot_index).astype(jnp.int32)
    repeated = jnp.repeat(embedded, TOPK, axis=0)
    buffer = jnp.zeros((EXPERTS * CAP, D), jnp.bfloat16).at[slot_dest].set(repeated)
    buffer = buffer.reshape(EXPERTS, CAP, D)

    def expert(operands):
        rows_in, gate_mat, up_mat, down_mat = operands
        gate_proj = jnp.dot(rows_in, gate_mat, preferred_element_type=jnp.float32)
        up_proj = jnp.dot(rows_in, up_mat, preferred_element_type=jnp.float32)
        hidden = (jax.nn.silu(gate_proj) * up_proj).astype(jnp.bfloat16)
        return jnp.dot(hidden, down_mat, preferred_element_type=jnp.float32)

    expert_out = lax.map(expert, (buffer, w_gate, w_up, w_down))
    picked = expert_out.reshape(EXPERTS * CAP, D)[slot_dest].reshape(TOKENS, TOPK, D)
    moe_out = jnp.sum(picked * gate_weights[:, :, None].astype(jnp.float32), axis=1)
    residual = (embedded.astype(jnp.float32) + moe_out).astype(jnp.bfloat16)
    block_width = D // N_EXPERT

    def add_block(total, block):
        start = (block * block_width).astype(jnp.int32)
        res_block = lax.dynamic_slice_in_dim(residual, start, block_width, 1)
        tab_block = lax.dynamic_slice_in_dim(embed_table, start, block_width, 1)
        part = lax.dot_general(res_block, tab_block, (((1,), (1,)), ((), ())), preferred_element_type=jnp.float32)
        rounded = lax.optimization_barrier(part.astype(jnp.bfloat16))
        return total + rounded.astype(jnp.float32), None

    start_total = jnp.zeros((TOKENS, VOC), jnp.float32)
    logits, unused = lax.scan(add_block, start_total, jnp.arange(N_EXPERT, dtype=jnp.int32))
    return logits.astype(jnp.bfloat16)
```

```python
import functools

import jax
import jax.numpy as jnp
from jax import lax
from jax.experimental import pallas as pl
from jax.experimental.pallas import tpu as pltpu
from jax.sharding import PartitionSpec as P

MESH = pl.DeviceIdType.MESH
GROUP = ("pipe", "vocab")


def peer_coords(axes, sizes, index):
    coords = {}
    for axis, size in reversed(list(zip(axes, sizes))):
        coords[axis] = index % size
        index = index // size
    return coords


def exchange_kernel(axes, sizes, reduce, x_ref, o_ref, *scratch):
    n = 1
    for size in sizes:
        n *= size
    me = 0
    for axis, size in zip(axes, sizes):
        me = me * size + lax.axis_index(axis)
    if reduce:
        land, send_sem, recv_sem = scratch
    else:
        land = o_ref
        send_sem, recv_sem, local_sem = scratch
    barrier = pltpu.get_barrier_semaphore()
    for k in range(1, n):
        where = peer_coords(axes, sizes, (me + k) % n)
        pl.semaphore_signal(barrier, inc=1, device_id=where, device_id_type=MESH)
    pl.semaphore_wait(barrier, n - 1)
    copies = []
    for k in range(1, n):
        peer = (me + k) % n
        copy = pltpu.make_async_remote_copy(
            src_ref=x_ref.at[peer] if reduce else x_ref,
            dst_ref=land.at[k - 1] if reduce else land.at[me],
            send_sem=send_sem.at[k - 1],
            recv_sem=recv_sem.at[k - 1],
            device_id=peer_coords(axes, sizes, peer),
            device_id_type=MESH,
        )
        copy.start()
        copies.append(copy)
    if not reduce:
        own = pltpu.make_async_copy(x_ref, land.at[me], local_sem)
        own.start()
        own.wait()
    for copy in copies:
        copy.wait()
    if reduce:
        columns = o_ref.shape[-1]
        tile = next((t for t in (512, 256, 128) if columns % t == 0), columns)

        @pl.loop(0, columns // tile)
        def _(step):
            cols = pl.ds(pl.multiple_of(step * tile, tile), tile)
            total = x_ref[me, :, cols].astype(jnp.float32)
            for k in range(n - 1):
                total = total + land[k, :, cols].astype(jnp.float32)
            o_ref[:, cols] = total.astype(o_ref.dtype)


def exchange(x, axes, reduce, collective_id, out_dtype=None):
    sizes = tuple(lax.axis_size(axis) for axis in axes)
    n = 1
    for size in sizes:
        n *= size
    block = x.shape[1:] if reduce else x.shape
    out = jax.ShapeDtypeStruct(block if reduce else (n,) + block, out_dtype or x.dtype)
    sems = [pltpu.SemaphoreType.DMA((n - 1,)), pltpu.SemaphoreType.DMA((n - 1,))]
    if reduce:
        scratch = [pltpu.VMEM((n - 1,) + block, x.dtype)] + sems
    else:
        scratch = sems + [pltpu.SemaphoreType.DMA]
    return pl.pallas_call(
        functools.partial(exchange_kernel, axes, sizes, reduce),
        out_shape=out,
        in_specs=[pl.BlockSpec(memory_space=pltpu.VMEM)],
        out_specs=pl.BlockSpec(memory_space=pltpu.VMEM),
        scratch_shapes=scratch,
        compiler_params=pltpu.CompilerParams(collective_id=collective_id, has_side_effects=True),
    )(x)


def per_device(token_ids, routes, gate_weights, embed_table, w_gate, w_up, w_down):
    vocab_rows, width_cols = embed_table.shape
    tokens = routes.shape[0]
    experts = lax.axis_size("expert")
    group = lax.axis_size(GROUP)
    width = experts * width_cols
    part = tokens // group
    row_base = lax.axis_index(GROUP) * vocab_rows
    local_ids = token_ids - row_base
    in_shard = (local_ids >= 0) & (local_ids < vocab_rows)
    rows = embed_table.at[jnp.clip(local_ids, 0, vocab_rows - 1)].get(mode="promise_in_bounds")
    rows = jnp.where(in_shard[:, None], rows, jnp.zeros_like(rows))
    own = exchange(rows.reshape(group, part, width_cols), GROUP, True, 0)
    wide = exchange(own, ("expert",), False, 1)
    wide = wide.transpose(1, 0, 2).reshape(part, width)
    embedded = exchange(wide, GROUP, False, 2).reshape(tokens, width)
    gate_proj = jnp.dot(embedded, w_gate[0], preferred_element_type=jnp.float32)
    up_proj = jnp.dot(embedded, w_up[0], preferred_element_type=jnp.float32)
    hidden = (jax.nn.silu(gate_proj) * up_proj).astype(jnp.bfloat16)
    share = jnp.sum(
        jnp.where(routes == lax.axis_index("expert"), gate_weights, 0.0), axis=1, keepdims=True
    )
    partial_out = jnp.dot(hidden, w_down[0], preferred_element_type=jnp.float32) * share
    partial_out = partial_out.astype(jnp.bfloat16).reshape(group, part, width)
    summed = exchange(partial_out, GROUP, True, 3)
    summed = summed.reshape(part, experts, width_cols).transpose(1, 0, 2)
    moe_out = exchange(summed, ("expert",), True, 4, jnp.float32)
    residual = (own.astype(jnp.float32) + moe_out).astype(jnp.bfloat16)
    residual = exchange(residual, GROUP, False, 5).reshape(tokens, width_cols)
    logits = lax.dot_general(
        residual, embed_table, (((1,), (1,)), ((), ())), preferred_element_type=jnp.float32
    ).astype(jnp.bfloat16)
    return exchange(logits.reshape(experts, tokens // experts, vocab_rows), ("expert",), True, 6)


def solution(mesh):
    return jax.shard_map(
        per_device,
        mesh=mesh,
        in_specs=(
            P(),
            P(),
            P(),
            P(GROUP, "expert"),
            P("expert", None, GROUP),
            P("expert", None, GROUP),
            P("expert", GROUP, None),
        ),
        out_specs=P("expert", GROUP),
        check_vma=False,
    )
```

```python
import functools

import jax
import jax.numpy as jnp
from jax import lax
from jax.experimental import pallas as pl
from jax.experimental.pallas import tpu as pltpu
from jax.sharding import PartitionSpec as P

MESH = pl.DeviceIdType.MESH
GROUP = ("pipe", "vocab")


def peer_coords(axes, sizes, index):
    coords = {}
    for axis, size in reversed(list(zip(axes, sizes))):
        coords[axis] = index % size
        index = index // size
    return coords


def exchange_kernel(axes, sizes, reduce, x_ref, o_ref, *scratch):
    n = 1
    for size in sizes:
        n *= size
    me = 0
    for axis, size in zip(axes, sizes):
        me = me * size + lax.axis_index(axis)
    if reduce:
        land, send_sem, recv_sem = scratch
    else:
        land = o_ref
        send_sem, recv_sem, local_sem = scratch
    barrier = pltpu.get_barrier_semaphore()
    for k in range(1, n):
        where = peer_coords(axes, sizes, (me + k) % n)
        pl.semaphore_signal(barrier, inc=1, device_id=where, device_id_type=MESH)
    pl.semaphore_wait(barrier, n - 1)
    copies = []
    for k in range(1, n):
        peer = (me + k) % n
        copy = pltpu.make_async_remote_copy(
            src_ref=x_ref.at[peer] if reduce else x_ref,
            dst_ref=land.at[k - 1] if reduce else land.at[me],
            send_sem=send_sem.at[k - 1],
            recv_sem=recv_sem.at[k - 1],
            device_id=peer_coords(axes, sizes, peer),
            device_id_type=MESH,
        )
        copy.start()
        copies.append(copy)
    if not reduce:
        own = pltpu.make_async_copy(x_ref, land.at[me], local_sem)
        own.start()
        own.wait()
    for copy in copies:
        copy.wait()
    if reduce:
        columns = o_ref.shape[-1]
        tile = next((t for t in (512, 256, 128) if columns % t == 0), columns)

        @pl.loop(0, columns // tile)
        def _(step):
            cols = pl.ds(pl.multiple_of(step * tile, tile), tile)
            total = x_ref[me, :, cols].astype(jnp.float32)
            for k in range(n - 1):
                total = total + land[k, :, cols].astype(jnp.float32)
            o_ref[:, cols] = total.astype(o_ref.dtype)


def exchange(x, axes, reduce, collective_id, out_dtype=None):
    sizes = tuple(lax.axis_size(axis) for axis in axes)
    n = 1
    for size in sizes:
        n *= size
    block = x.shape[1:] if reduce else x.shape
    out = jax.ShapeDtypeStruct(block if reduce else (n,) + block, out_dtype or x.dtype)
    sems = [pltpu.SemaphoreType.DMA((n - 1,)), pltpu.SemaphoreType.DMA((n - 1,))]
    if reduce:
        scratch = [pltpu.VMEM((n - 1,) + block, x.dtype)] + sems
    else:
        scratch = sems + [pltpu.SemaphoreType.DMA]
    return pl.pallas_call(
        functools.partial(exchange_kernel, axes, sizes, reduce),
        out_shape=out,
        in_specs=[pl.BlockSpec(memory_space=pltpu.VMEM)],
        out_specs=pl.BlockSpec(memory_space=pltpu.VMEM),
        scratch_shapes=scratch,
        compiler_params=pltpu.CompilerParams(collective_id=collective_id, has_side_effects=True),
    )(x)


def core_pair_kernel(sizes, reduce, x_ref, o_ref, *scratch):
    pipes, vocabs = sizes
    p, v = lax.axis_index("pipe"), lax.axis_index("vocab")
    core, me = p % 2, p * vocabs + v
    chips = pipes * vocabs // 2
    chip = (p // 2) * vocabs + v
    other = {"pipe": p + 1 - 2 * core, "vocab": v}

    def of_chip(index, on):
        pipe = (index // vocabs) * 2 + on
        return {"pipe": pipe, "vocab": index % vocabs}, pipe * vocabs + index % vocabs

    def send(src, dst, sems, at, where):
        copy = pltpu.make_async_remote_copy(
            src_ref=src, dst_ref=dst, send_sem=sems.at[0, at], recv_sem=sems.at[1, at],
            device_id=where, device_id_type=MESH,
        )
        copy.start()
        return copy

    barrier = pltpu.get_barrier_semaphore()
    pl.semaphore_signal(barrier, inc=1, device_id=other, device_id_type=MESH)
    for k in range(1, chips):
        where, _ = of_chip((chip + k) % chips, core)
        pl.semaphore_signal(barrier, inc=1, device_id=where, device_id_type=MESH)
    pl.semaphore_wait(barrier, chips)
    if not reduce:
        far, near, local_sem = scratch
        outgoing = []
        for k in range(1, chips):
            where, _ = of_chip((chip + k) % chips, core)
            outgoing.append(send(x_ref, o_ref.at[me], far, k, where))
        passed = [send(x_ref, o_ref.at[me], near, 0, other)]
        own = pltpu.make_async_copy(x_ref, o_ref.at[me], local_sem)
        own.start()
        for k in range(1, chips):
            outgoing[k - 1].wait_recv()
            _, source = of_chip((chip + chips - k) % chips, core)
            passed.append(send(o_ref.at[source], o_ref.at[source], near, k, other))
        own.wait()
        for copy in outgoing:
            copy.wait_send()
        for copy in passed:
            copy.wait()
        return
    paired, merged, land, far, near = scratch
    columns = o_ref.shape[-1]
    tile = next((t for t in (512, 256, 128) if columns % t == 0), columns)

    def each_tile(body):
        @pl.loop(0, columns // tile)
        def _(step):
            body(pl.ds(pl.multiple_of(step * tile, tile), tile))

    given = []
    order = list(range(1, chips)) + [0]
    for k in order:
        _, index = of_chip((chip + k) % chips, 1 - core)
        given.append(send(x_ref.at[index], paired.at[k], near, k, other))
    outgoing, ready = [], None
    for copy, k in zip(given, order):
        copy.wait_recv()
        where, index = of_chip((chip + k) % chips, core)

        def merge(cols):
            total = x_ref[index, :, cols].astype(jnp.float32)
            total = total + paired[k, :, cols].astype(jnp.float32)
            merged[k, :, cols] = total.astype(merged.dtype)

        if k:
            each_tile(merge)
        if ready is not None:
            at, to = ready
            outgoing.append(send(merged.at[at], land.at[at], far, at, to))
        ready = (k, where)
    for copy in given:
        copy.wait_send()
    for copy in outgoing:
        copy.wait()

    def finish(cols):
        total = x_ref[me, :, cols].astype(jnp.float32) + paired[0, :, cols].astype(jnp.float32)
        for k in range(1, chips):
            total = total + land[k, :, cols].astype(jnp.float32)
        o_ref[:, cols] = total.astype(o_ref.dtype)

    each_tile(finish)


def core_pair_exchange(x, reduce, collective_id):
    sizes = tuple(lax.axis_size(axis) for axis in GROUP)
    n = sizes[0] * sizes[1]
    chips = n // 2
    block = x.shape[1:] if reduce else x.shape
    pair_sems = [pltpu.SemaphoreType.DMA((2, chips)), pltpu.SemaphoreType.DMA((2, chips))]
    if reduce:
        scratch = [pltpu.VMEM((chips,) + block, x.dtype)] * 3 + pair_sems
    else:
        scratch = pair_sems + [pltpu.SemaphoreType.DMA]
    return pl.pallas_call(
        functools.partial(core_pair_kernel, sizes, reduce),
        out_shape=jax.ShapeDtypeStruct(block if reduce else (n,) + block, x.dtype),
        in_specs=[pl.BlockSpec(memory_space=pltpu.VMEM)],
        out_specs=pl.BlockSpec(memory_space=pltpu.VMEM),
        scratch_shapes=scratch,
        compiler_params=pltpu.CompilerParams(collective_id=collective_id, has_side_effects=True),
    )(x)


def logits_kernel(n, steps, x_ref, table_ref, o_ref, held, land, send_sem, recv_sem):
    step = pl.program_id(0)
    me = lax.axis_index("expert")
    part, tile = held.shape[1], table_ref.shape[0]

    def sends(at):
        cols = pl.ds(pl.multiple_of(at * tile, tile), tile)
        return [
            pltpu.make_async_remote_copy(
                src_ref=held.at[(me + k) % n, :, cols],
                dst_ref=land.at[k - 1, :, cols],
                send_sem=send_sem.at[k - 1, at],
                recv_sem=recv_sem.at[k - 1, at],
                device_id={"expert": (me + k) % n},
                device_id_type=MESH,
            )
            for k in range(1, n)
        ]

    @pl.when(step == 0)
    def _():
        barrier = pltpu.get_barrier_semaphore()
        for k in range(1, n):
            pl.semaphore_signal(
                barrier, inc=1, device_id={"expert": (me + k) % n}, device_id_type=MESH
            )
        pl.semaphore_wait(barrier, n - 1)

    @pl.when(step > 0)
    def _():
        for copy in sends(step - 1):
            copy.start()

    block = lax.dot_general(
        x_ref[...], table_ref[...], (((1,), (1,)), ((), ())), preferred_element_type=jnp.float32
    ).astype(held.dtype)
    here = pl.ds(pl.multiple_of(step * tile, tile), tile)
    for i in range(n):
        held[i, :, here] = block[i * part : (i + 1) * part]

    @pl.when(step == steps - 1)
    def _():
        for copy in sends(steps - 1):
            copy.start()

        @pl.loop(0, steps)
        def _(at):
            for copy in sends(at):
                copy.wait()
            cols = pl.ds(pl.multiple_of(at * tile, tile), tile)
            total = held[me, :, cols].astype(jnp.float32)
            for k in range(n - 1):
                total = total + land[k, :, cols].astype(jnp.float32)
            o_ref[:, cols] = total.astype(o_ref.dtype)


def logits_sum(residual, table, collective_id):
    n = lax.axis_size("expert")
    (tokens, width), rows = residual.shape, table.shape[0]
    part, tile = tokens // n, 512
    steps = rows // tile
    return pl.pallas_call(
        functools.partial(logits_kernel, n, steps),
        grid=(steps,),
        out_shape=jax.ShapeDtypeStruct((part, rows), residual.dtype),
        in_specs=[
            pl.BlockSpec((tokens, width), lambda i: (0, 0)),
            pl.BlockSpec((tile, width), lambda i: (i, 0)),
        ],
        out_specs=pl.BlockSpec((part, rows), lambda i: (0, 0)),
        scratch_shapes=[
            pltpu.VMEM((n, part, rows), residual.dtype),
            pltpu.VMEM((n - 1, part, rows), residual.dtype),
            pltpu.SemaphoreType.DMA((n - 1, steps)),
            pltpu.SemaphoreType.DMA((n - 1, steps)),
        ],
        compiler_params=pltpu.CompilerParams(
            collective_id=collective_id, has_side_effects=True,
            dimension_semantics=("arbitrary",),
        ),
    )(residual, table)


def per_device(token_ids, routes, gate_weights, embed_table, w_gate, w_up, w_down):
    vocab_rows, width_cols = embed_table.shape
    tokens = routes.shape[0]
    experts = lax.axis_size("expert")
    group = lax.axis_size(GROUP)
    width = experts * width_cols
    part = tokens // group
    row_base = lax.axis_index(GROUP) * vocab_rows
    local_ids = token_ids - row_base
    in_shard = (local_ids >= 0) & (local_ids < vocab_rows)
    rows = embed_table.at[jnp.clip(local_ids, 0, vocab_rows - 1)].get(mode="promise_in_bounds")
    rows = jnp.where(in_shard[:, None], rows, jnp.zeros_like(rows))
    own = exchange(rows.reshape(group, part, width_cols), GROUP, True, 0)
    wide = exchange(own, ("expert",), False, 1)
    wide = wide.transpose(1, 0, 2).reshape(part, width)
    embedded = core_pair_exchange(wide, False, 2).reshape(tokens, width)
    gate_proj = jnp.dot(embedded, w_gate[0], preferred_element_type=jnp.float32)
    up_proj = jnp.dot(embedded, w_up[0], preferred_element_type=jnp.float32)
    hidden = (jax.nn.silu(gate_proj) * up_proj).astype(jnp.bfloat16)
    share = jnp.sum(
        jnp.where(routes == lax.axis_index("expert"), gate_weights, 0.0), axis=1, keepdims=True
    )
    partial_out = jnp.dot(hidden, w_down[0], preferred_element_type=jnp.float32) * share
    partial_out = partial_out.astype(jnp.bfloat16).reshape(group, part, width)
    summed = core_pair_exchange(partial_out, True, 3)
    summed = summed.reshape(part, experts, width_cols).transpose(1, 0, 2)
    moe_out = exchange(summed, ("expert",), True, 4, jnp.float32)
    residual = (own.astype(jnp.float32) + moe_out).astype(jnp.bfloat16)
    residual = exchange(residual, GROUP, False, 5).reshape(tokens, width_cols)
    return logits_sum(residual, embed_table, 6)


def solution(mesh):
    return jax.shard_map(
        per_device,
        mesh=mesh,
        in_specs=(
            P(),
            P(),
            P(),
            P(GROUP, "expert"),
            P("expert", None, GROUP),
            P("expert", None, GROUP),
            P("expert", GROUP, None),
        ),
        out_specs=P("expert", GROUP),
        check_vma=False,
    )
```
